256 devices in a mesh: tm: 4 (over x_hi, core), chan: 64 (over x_lo, y, z).
Axes of the slice: x: 4 (x_hi: 2, x_lo: 2; x = x_hi * 2 + x_lo), y: 4, z: 8, core: 2. Of those that a mesh axis runs over, the one named last changes fastest.
Arguments:
- raw: bfloat16 [4096, 131072], P('chan', 'tm'), may hold values from -6 to 6
- starts: int32 [32], P('tm'), may hold values from 0 to 28672
- dead_mask: int32 [4096], P('chan'), may hold values 0 or 1
- offsets: int32 [16], replicated, may hold values from 1 to 256, as said below
Outputs:
- correlations: float32 [16, 4096, 256], P('tm', 'chan')
The draws below stay inside these ranges and needn't reach their ends.
Inputs may be any that keep to these rules, and one draw needn't show every extreme that they name: `offsets`: the entries are distinct, and 256 is always one of them.
All inputs are finite; a program needn't handle non-finite values. No bound on the sum of `dead_mask` on one device may be relied on, other than what follows from the above.
Results may differ from the reference program's by a relative error of at most 0.0049.
Values may be sent and summed in bfloat16 or wider, within the bound.
No kernel may reach another device: no remote copies, remote signals or barrier semaphores. Data moves between devices by JAX's collectives and lax.ppermute only.
A program may use at most 128 MiB of HBM per device.

```python
import jax
import jax.numpy as jnp
from jax import lax

W_DEV = 8
HOP = 4096
F = 640
F0 = 16
LAGS = 256
MAXOFF = 256
NOFF = 16
WIN = 8192
CH = 4096
WINDOWS = 32
SAMPLES = 131072


def draw_offsets(key, part):
    chosen = jax.random.permutation(jax.random.fold_in(key, 11), MAXOFF - 1).astype(jnp.int32) + 1
    values = jnp.concatenate([chosen[:NOFF - 1], jnp.full((1,), MAXOFF, jnp.int32)])
    order = jax.random.permutation(jax.random.fold_in(key, 23), NOFF)
    return values[order].astype(jnp.int32)


def touch_ends(drawn, key, low, top_value):
    index_at = [jax.random.randint(jax.random.fold_in(key, axis), (), 0, length) for axis, length in enumerate(drawn.shape)]
    longest = drawn.shape.index(max(drawn.shape))
    neighbour = index_at[:longest] + [(index_at[longest] + 1) % drawn.shape[longest]] + index_at[longest + 1:]
    return drawn.at[tuple(index_at)].set(low).at[tuple(neighbour)].set(top_value)


def block_scale(key, extent, shards, low, high):
    gain = 1.0
    for position, shards_of in shards:
        steps = jax.random.uniform(jax.random.fold_in(jax.random.fold_in(key, 6), position), (shards_of,), jnp.float32, low / len(shards), high / len(shards))
        gain = gain * jnp.repeat(jnp.exp(steps), extent[position] // shards_of).reshape((-1,) + (1,) * (len(extent) - 1 - position))
    return gain


def bell_draw(stream_key, shape, deviation, bound, shards=(), held_as=jnp.bfloat16):
    result = deviation * jax.random.normal(stream_key, shape, jnp.float32)
    if shards:
        result = result * block_scale(stream_key, shape, shards, -0.22, 0.18)
    return jnp.clip(result, -bound, bound).astype(held_as)


def setup_inputs(seed: int = 0) -> dict:
    key_of = jax.random.split(jax.random.key(seed), 5)
    return {
        "raw": bell_draw(key_of[0], (CH, SAMPLES), 1.0, 6.0, ((0, 64), (1, 4))),
        "starts": touch_ends(jax.random.randint(key_of[1], (WINDOWS,), 0, (W_DEV - 1) * HOP + 1), jax.random.fold_in(key_of[1], 1), 0, (W_DEV - 1) * HOP).astype(jnp.int32),
        "dead_mask": touch_ends((jax.random.randint(key_of[2], (CH,), 0, 8) < 7).astype(jnp.int32), jax.random.fold_in(key_of[2], 1), 0, 1),
        "offsets": draw_offsets(jax.random.fold_in(key_of[4], 71), 0),
    }


def forward_table(first, count):
    sample = jnp.arange(count, dtype=jnp.int32) + first
    bins = jnp.arange(F, dtype=jnp.int32) + F0
    phase = sample[:, None] * bins[None, :] % WIN
    angle = 2.0 * jnp.pi / WIN * phase.astype(jnp.float32)
    return jnp.concatenate([jnp.cos(angle), -jnp.sin(angle)], axis=1).astype(jnp.bfloat16)

def inverse_table():
    bins = jnp.arange(F, dtype=jnp.int32) + F0
    lagged = jnp.arange(LAGS, dtype=jnp.int32) - LAGS // 2
    phase = jnp.mod(bins[:, None] * lagged[None, :], WIN)
    angle = 2.0 * jnp.pi / WIN * phase.astype(jnp.float32)
    return jnp.concatenate([jnp.cos(angle), -jnp.sin(angle)], axis=0)

def whiten(spectrum, live):
    real_part = spectrum[..., :F]
    imag_part = spectrum[..., F:]
    amplitude = jnp.sqrt(real_part * real_part + imag_part * imag_part)
    level = lax.optimization_barrier(jnp.mean(amplitude, axis=-1, keepdims=True))
    scaled = 1.0 / (amplitude + 0.1 * level + 1e-06)
    scaled = jnp.concatenate([scaled, scaled], axis=-1)
    return (spectrum * scaled * live[:, None]).astype(jnp.bfloat16)

def reference(raw, starts, dead_mask, offsets):
    padded = jnp.concatenate([raw, jnp.zeros((CH, HOP), jnp.bfloat16)], axis=1)
    group = jnp.arange(WINDOWS, dtype=jnp.int32) // W_DEV
    begin = (group * (W_DEV * HOP) + starts).astype(jnp.int32)
    hann = 0.5 - 0.5 * jnp.cos(2.0 * jnp.pi * jnp.arange(WIN, dtype=jnp.float32) / WIN)
    table = forward_table(0, WIN)
    live = dead_mask.astype(jnp.float32)

    def one_window(first):
        segment = lax.dynamic_slice_in_dim(padded, first, WIN, 1)
        tapered = (segment.astype(jnp.float32) * hann[None, :]).astype(jnp.bfloat16)
        spectrum = jnp.dot(tapered, table, preferred_element_type=jnp.float32)
        return whiten(spectrum, live)
    white = lax.map(one_window, begin)
    extended = jnp.concatenate([white, jnp.zeros((WINDOWS, MAXOFF, 2 * F), jnp.bfloat16)], axis=1)
    back = inverse_table()
    scale = 1.0 / jnp.sqrt(jnp.float32(WINDOWS * F))
    own = white.astype(jnp.float32)

    def one_offset(distance):
        partner = lax.dynamic_slice_in_dim(extended, distance.astype(jnp.int32), CH, 1).astype(jnp.float32)
        a_re, a_im = (own[..., :F], own[..., F:])
        b_re, b_im = (partner[..., :F], partner[..., F:])
        stack_re = lax.optimization_barrier(jnp.sum(a_re * b_re + a_im * b_im, axis=0))
        stack_im = lax.optimization_barrier(jnp.sum(a_im * b_re - a_re * b_im, axis=0))
        stack = jnp.concatenate([stack_re, stack_im], axis=1)
        return jnp.dot(stack, back, precision=lax.Precision.HIGHEST, preferred_element_type=jnp.float32) * scale
    return lax.map(one_offset, offsets)
```

```python
import jax
import jax.numpy as jnp
import numpy as np
from jax import lax
from jax.experimental import pallas as pl
from jax.experimental.pallas import tpu as pltpu
from jax.sharding import PartitionSpec as P

HOP = 4096
WIN = 8192
F = 640
F0 = 16
LAGS = 256
W_DEV = 8
TILE = 128
HALF = 384
SEED = 64
STEPS = 8
CHUNKS = 2


def half_bins():
    even = np.arange(F0, F0 + F, 2)
    odd = np.arange(F0 + 1, F0 + F, 2)
    pad = np.full(HALF - F // 2, -1)
    return np.concatenate([even, pad]), np.concatenate([pad, odd])


def seeds(bins):
    used = (bins >= 0).astype(np.float64)
    fine = 2 * np.pi / WIN * (np.arange(SEED)[:, None] * bins[None, :] % WIN)
    coarse = 2 * np.pi / WIN * (SEED * np.arange(HOP // SEED)[:, None] * bins[None, :] % WIN)
    parts = np.cos(fine) * used, np.sin(fine) * used, np.cos(coarse), np.sin(coarse)
    return [part.astype(np.float32) for part in parts]


def half_table(bins):
    c1, s1, c2, s2 = seeds(bins)
    c1, s1 = c1[None], s1[None]
    c2, s2 = c2[:, None], s2[:, None]
    cosine = c1 * jnp.asarray(c2) - s1 * jnp.asarray(s2)
    sine = s1 * jnp.asarray(c2) + c1 * jnp.asarray(s2)
    return jnp.concatenate([cosine, -sine], axis=-1).astype(jnp.bfloat16).reshape(HOP, 2 * HALF)


def inverse_table():
    bins = np.concatenate([np.arange(F0, F0 + F, 2), np.arange(F0 + 1, F0 + F, 2)])
    lagged = np.arange(LAGS) - LAGS // 2
    angle = 2 * np.pi / WIN * (bins[:, None] * lagged[None, :] % WIN)
    return np.concatenate([np.cos(angle), -np.sin(angle)], axis=0).astype(jnp.bfloat16)


def spectra_kernel(starts, raw, after, hann, live, even, odd, out, padded, acc, sems):
    step = pl.program_id(0)
    rows = raw.shape[0]
    width = HOP // STEPS
    count = out.shape[0]

    @pl.when(step == 0)
    def _():
        span = raw.shape[1]
        first = pltpu.make_async_copy(raw, padded.at[:, pl.ds(0, span)], sems.at[0])
        second = pltpu.make_async_copy(after, padded.at[:, pl.ds(span, HOP)], sems.at[1])
        first.start()
        second.start()
        first.wait()
        second.wait()
        acc[...] = jnp.zeros_like(acc)

    lane = lax.broadcasted_iota(jnp.int32, (1, width), 1)
    sums, differences = [], []
    for w in range(count):
        block = starts[w] // WIN * WIN
        inside = starts[w] % WIN
        tapered = []
        for half in range(2):
            at = pl.multiple_of(half * HOP + step * width, width)
            here = padded[:, pl.ds(pl.multiple_of(block + at, width), width)].astype(jnp.float32)
            later = padded[:, pl.ds(pl.multiple_of(block + WIN + at, width), width)].astype(jnp.float32)
            picked = jnp.where(lane + at >= inside, here, later) * hann[pl.ds(w, 1), pl.ds(at, width)]
            tapered.append(picked.astype(jnp.bfloat16).astype(jnp.float32))
        sums.append((tapered[0] + tapered[1]).astype(jnp.bfloat16))
        differences.append((tapered[0] - tapered[1]).astype(jnp.bfloat16))
    low = jnp.dot(jnp.concatenate(sums, axis=0), even[...], preferred_element_type=jnp.float32)
    high = jnp.dot(jnp.concatenate(differences, axis=0), odd[...], preferred_element_type=jnp.float32)
    acc[:, 0:HALF] += low[:, :HALF]
    acc[:, F : F + HALF] += low[:, HALF:]
    acc[:, F - HALF : F] += high[:, :HALF]
    acc[:, 2 * F - HALF : 2 * F] += high[:, HALF:]

    @pl.when(step == STEPS - 1)
    def _():
        for w in range(count):
            real = acc[pl.ds(w * rows, rows), 0:F]
            imag = acc[pl.ds(w * rows, rows), F : 2 * F]
            amplitude = jnp.sqrt(real * real + imag * imag)
            level = jnp.mean(amplitude, axis=-1, keepdims=True)
            scaled = live[...] / (amplitude + 0.1 * level + 1e-06)
            out[w, :, 0:F] = (real * scaled).astype(jnp.bfloat16)
            out[w, :, F : 2 * F] = (imag * scaled).astype(jnp.bfloat16)


def spectra(starts, raw, after, hann, live, even, odd):
    rows, span = raw.shape
    count = starts.shape[0]
    width = HOP // STEPS
    table = pl.BlockSpec((width, 2 * HALF), lambda k, s: (k, 0))
    return pl.pallas_call(
        spectra_kernel,
        grid_spec=pltpu.PrefetchScalarGridSpec(
            num_scalar_prefetch=1,
            grid=(STEPS,),
            in_specs=[
                pl.BlockSpec(memory_space=pl.ANY),
                pl.BlockSpec(memory_space=pl.ANY),
                pl.BlockSpec((count, WIN), lambda k, s: (0, 0)),
                pl.BlockSpec((rows, 1), lambda k, s: (0, 0)),
                table,
                table,
            ],
            out_specs=pl.BlockSpec((count, rows, 2 * F), lambda k, s: (0, 0, 0)),
            scratch_shapes=[
                pltpu.VMEM((rows, span + WIN), jnp.bfloat16),
                pltpu.VMEM((count * rows, 2 * F), jnp.float32),
                pltpu.SemaphoreType.DMA((2,)),
            ],
        ),
        out_shape=jax.ShapeDtypeStruct((count, rows, 2 * F), jnp.bfloat16),
        compiler_params=pltpu.CompilerParams(vmem_limit_bytes=32 << 20),
        cost_estimate=pl.CostEstimate(flops=2 * count * rows * HOP * 4 * HALF, bytes_accessed=20 << 20, transcendentals=0),
        name="spectra",
    )(starts, raw, after, hann, live, even, odd)


def correlate_kernel(offsets, *refs):
    blocks = refs[:5]
    table, rest = refs[5], refs[6:]
    out, wide, stack = rest[-3:]
    count, rows, _ = blocks[0].shape
    tiles = 2 * F // TILE
    for at, block in enumerate(blocks):
        for w in range(count):
            for tile in range(tiles):
                wide[w, tile, pl.ds(at * rows, rows), :] = block[w, :, pl.ds(tile * TILE, TILE)].astype(jnp.float32)
    group = 16

    def one_offset(o, carry):
        distance = offsets[o]
        mine = jnp.where(distance >= 2 * rows, 0, 2 * rows)
        theirs = mine + distance
        for part in range(rows // group):
            for tile in range(tiles // 2):
                real = jnp.zeros((group, TILE), jnp.float32)
                imag = jnp.zeros((group, TILE), jnp.float32)
                for w in range(count):
                    at = pl.multiple_of(mine + part * group, group)
                    a_re = wide[w, tile, pl.ds(at, group), :]
                    a_im = wide[w, tile + tiles // 2, pl.ds(at, group), :]
                    b_re = wide[w, tile, pl.ds(theirs + part * group, group), :]
                    b_im = wide[w, tile + tiles // 2, pl.ds(theirs + part * group, group), :]
                    real = real + a_re * b_re + a_im * b_im
                    imag = imag + a_im * b_re - a_re * b_im
                row = pl.ds(pl.multiple_of(o * rows + part * group, group), group)
                stack[row, pl.ds(tile * TILE, TILE)] = real.astype(jnp.bfloat16)
                stack[row, pl.ds(F + tile * TILE, TILE)] = imag.astype(jnp.bfloat16)
        return carry

    lax.fori_loop(0, offsets.shape[0], one_offset, 0)
    for part in range(4):
        row = pl.ds(part * (stack.shape[0] // 4), stack.shape[0] // 4)
        value = jnp.dot(stack[row, :], table[...], preferred_element_type=jnp.float32)
        if len(rest) == 4:
            value = value + rest[0][row, :]
        out[row, :] = value.astype(out.dtype)


def correlate(offsets, blocks, table, earlier, dtype):
    count, rows, _ = blocks[0].shape
    total = offsets.shape[0] * rows
    more = [] if earlier is None else [earlier]
    vmem = pl.BlockSpec(memory_space=pltpu.VMEM)
    return pl.pallas_call(
        correlate_kernel,
        in_specs=[pl.BlockSpec(memory_space=pltpu.SMEM)] + [vmem] * (6 + len(more)),
        out_specs=vmem,
        out_shape=jax.ShapeDtypeStruct((total, LAGS), dtype),
        scratch_shapes=[
            pltpu.VMEM((count, 2 * F // TILE, 5 * rows, TILE), jnp.float32),
            pltpu.VMEM((total, 2 * F), jnp.bfloat16),
        ],
        compiler_params=pltpu.CompilerParams(vmem_limit_bytes=32 << 20),
        cost_estimate=pl.CostEstimate(flops=2 * total * 2 * F * LAGS, bytes_accessed=8 << 20, transcendentals=0),
        name="correlate",
    )(offsets, *blocks, table, *more)


def moved(block, axis, distance):
    size = lax.axis_size(axis)
    return lax.ppermute(block, axis, [(i, i + distance) for i in range(size) if 0 <= i + distance < size])


def local(raw, starts, dead_mask, offsets):
    rows = raw.shape[0]
    windows = starts.shape[0]
    after = moved(raw[:, :HOP], "tm", -1)
    phase = (jnp.arange(WIN, dtype=jnp.int32)[None, :] - starts[:, None]) & (WIN - 1)
    hann = 0.5 - 0.5 * jnp.cos(2.0 * jnp.pi * phase.astype(jnp.float32) / WIN)
    live = dead_mask.astype(jnp.float32)[:, None]
    even_bins, odd_bins = half_bins()
    even, odd = half_table(even_bins), half_table(odd_bins)
    back = jnp.asarray(inverse_table())

    size = windows // CHUNKS
    own, left, right = [], [], []
    for c in range(CHUNKS):
        part = slice(c * size, (c + 1) * size)
        own.append(spectra(starts[part], raw, after, hann[part], live, even, odd))
        left.append(moved(own[c], "chan", 1))
        right.append(moved(own[c], "chan", -1))
    total = None
    for c in range(CHUNKS):
        far_left, far_right = moved(left[c], "chan", 1), moved(right[c], "chan", -1)
        last = c == CHUNKS - 1
        total = correlate(
            offsets, [far_left, left[c], own[c], right[c], far_right], back, total, jnp.bfloat16 if last else jnp.float32
        )

    owners = lax.axis_size("tm")
    each = offsets.shape[0] // owners
    me = lax.axis_index("tm")
    core, side = me % 2, me // 2
    split = total.reshape(2, 2, each, rows, LAGS)
    sent = lax.dynamic_index_in_dim(split, 1 - core, 1, keepdims=False)
    kept = lax.dynamic_index_in_dim(split, core, 1, keepdims=False)
    got = lax.ppermute(sent, "tm", [(i, i ^ 1) for i in range(owners)])
    pair = kept.astype(jnp.float32) + got.astype(jnp.float32)
    sent = lax.dynamic_index_in_dim(pair, 1 - side, 0, keepdims=False).astype(jnp.bfloat16)
    kept = lax.dynamic_index_in_dim(pair, side, 0, keepdims=False)
    got = lax.ppermute(sent, "tm", [(i, i ^ 2) for i in range(owners)])
    scale = 1.0 / jnp.sqrt(jnp.float32(windows * owners * F))
    result = (kept + got.astype(jnp.float32)) * scale
    ahead = moved(result.astype(jnp.bfloat16), "chan", -2)
    mine = lax.dynamic_slice_in_dim(offsets, me * each, each)
    return jnp.where((mine >= 2 * rows)[:, None, None], ahead.astype(jnp.float32), result)


def solution(mesh):
    in_specs = (P("chan", "tm"), P("tm"), P("chan"), P())
    out_specs = P("tm", "chan", None)
    return jax.shard_map(local, mesh=mesh, in_specs=in_specs, out_specs=out_specs, check_vma=False)
```

```python
import functools

import jax
import jax.numpy as jnp
import numpy as np
from jax import lax
from jax.experimental import pallas as pl
from jax.experimental.pallas import tpu as pltpu
from jax.sharding import PartitionSpec as P

HOP = 4096
WIN = 8192
F = 640
F0 = 16
LAGS = 256
W_DEV = 8
TILE = 128
RADIX = 8
ORDER = (1, 7, 2, 6, 3, 5, 0, 4)
SPAN = WIN // RADIX
PAIRS = RADIX // 2
PAIR = F // PAIRS
SEED = 64
CHUNKS = (3, 3, 2)


def ordered_bins():
    return np.concatenate([np.arange(F0 + branch, F0 + F, RADIX) for branch in ORDER])


def forward_tables():
    bins = ordered_bins()
    spread = np.full((PAIRS, 2 * TILE), -1)
    for pair in range(PAIRS):
        at = pair * (PAIR - TILE)
        spread[pair, at : at + PAIR] = bins[pair * PAIR : (pair + 1) * PAIR]
    spread = spread.reshape(-1)
    near = 2 * np.pi / WIN * (np.arange(SEED)[:, None] * spread[None, :] % WIN)
    far = 2 * np.pi / WIN * (SEED * np.arange(SPAN // SEED)[:, None] * spread[None, :] % WIN)
    used = spread >= 0
    c1, s1 = (jnp.asarray(part * used, jnp.float32)[None] for part in (np.cos(near), np.sin(near)))
    c2, s2 = (jnp.asarray(part, jnp.float32)[:, None] for part in (np.cos(far), np.sin(far)))
    return [part.astype(jnp.bfloat16).reshape(SPAN, -1) for part in (c1 * c2 - s1 * s2, s1 * c2 + c1 * s2)]


def inverse_table():
    bins = ordered_bins()
    lagged = np.arange(LAGS) - LAGS // 2
    angle = 2 * np.pi / WIN * (bins[:, None] * lagged[None, :] % WIN)
    return np.concatenate([np.cos(angle), -np.sin(angle)], axis=0).astype(jnp.bfloat16)


def branches(x):
    total = [x[j] + x[j + 4] for j in range(4)]
    apart = [x[j] - x[j + 4] for j in range(4)]
    even, odd = total[0] + total[2], total[1] + total[3]
    side = (apart[1] - apart[3]) * np.float32(np.sqrt(0.5))
    down = (apart[1] + apart[3]) * np.float32(np.sqrt(0.5))
    return [
        (apart[0] + side, -apart[2] - down),
        (total[0] - total[2], total[3] - total[1]),
        (apart[0] - side, apart[2] - down),
        (even + odd, even - odd),
    ]


def spectra_kernel(begin, starts, raw, after, dead, cosine, sine, *refs):
    out, folded, product = refs[-3:]
    rows, span = raw.shape
    count = out.shape[0]
    last = span - WIN
    group, width = 16, 2 * TILE

    place = lax.broadcasted_iota(jnp.int32, (RADIX, SPAN), 0) * SPAN + lax.broadcasted_iota(jnp.int32, (RADIX, SPAN), 1)

    def fold(w, carry):
        start = starts[begin + w]
        block = pl.multiple_of(start // WIN * WIN, WIN)
        inside = start % WIN
        after_block = pl.multiple_of(jnp.minimum(block + WIN, last), WIN)
        phase = (place - start) & (WIN - 1)
        hann = 0.5 - 0.5 * jnp.cos(np.float32(2 * np.pi / WIN) * phase.astype(jnp.float32))
        for at in range(0, SPAN, width):
            lane = lax.broadcasted_iota(jnp.int32, (group, width), 1) + at
            for row in range(0, rows, group):
                x = []
                for j in range(RADIX):
                    here = raw[pl.ds(row, group), pl.ds(block + j * SPAN + at, width)]
                    later = raw[pl.ds(row, group), pl.ds(after_block + j * SPAN + at, width)]
                    if j * SPAN < HOP:
                        later = jnp.where(block == last, after[pl.ds(row, group), pl.ds(j * SPAN + at, width)], later)
                    picked = jnp.where(lane >= inside - j * SPAN, here.astype(jnp.float32), later.astype(jnp.float32))
                    picked = picked * hann[j : j + 1, at : at + width]
                    x.append(picked.astype(jnp.bfloat16).astype(jnp.float32))
                for pair, values in enumerate(branches(x)):
                    for part, value in enumerate(values):
                        to = pl.multiple_of((part * count + w) * rows + row, group)
                        folded[pair, pl.ds(to, group), pl.ds(at, width)] = value.astype(jnp.bfloat16)
        return carry

    lax.fori_loop(0, count, fold, 0)
    for pair in range(PAIRS):
        columns = slice(pair * width, (pair + 1) * width)
        product[pair, 0] = jnp.dot(folded[pair], cosine[:, columns], preferred_element_type=jnp.float32)
        product[pair, 1] = jnp.dot(folded[pair], sine[:, columns], preferred_element_type=jnp.float32)

    square = lax.broadcasted_iota(jnp.int32, (rows, rows), 0) == lax.broadcasted_iota(jnp.int32, (rows, rows), 1)
    live = jnp.sum(jnp.where(square, dead[...].astype(jnp.float32), 0.0), axis=1, keepdims=True)
    lane = lax.broadcasted_iota(jnp.int32, (1, width), 1)
    for w in range(count):
        first, second = pl.ds(w * rows, rows), pl.ds((count + w) * rows, rows)
        reals, imags = [], []
        for pair in range(PAIRS):
            leading = lane < pair * (PAIR - TILE) + PAIR // 2
            c_first, c_second = product[pair, 0, first, :], product[pair, 0, second, :]
            s_first, s_second = product[pair, 1, first, :], product[pair, 1, second, :]
            if pair < PAIRS - 1:
                reals.append(c_first + jnp.where(leading, s_second, -s_second))
                imags.append(jnp.where(leading, c_second, -c_second) - s_first)
            else:
                reals.append(jnp.where(leading, c_first, c_second))
                imags.append(-jnp.where(leading, s_first, s_second))
        tiles = [[], []]
        for into, parts in zip(tiles, (reals, imags)):
            into.append(parts[0][:, :TILE])
            for pair in range(1, PAIRS):
                into.append(parts[pair - 1][:, TILE:] + parts[pair][:, :TILE])
            into.append(parts[-1][:, TILE:])
        sizes = [jnp.sqrt(re * re + im * im) for re, im in zip(*tiles)]
        level = jnp.sum(sum(sizes[1:], sizes[0]), axis=-1, keepdims=True) * np.float32(1 / F)
        for tile, (re, im, amplitude) in enumerate(zip(*tiles, sizes)):
            scaled = live / (amplitude + 0.1 * level + 1e-06)
            out[w, :, pl.ds(tile * TILE, TILE)] = (re * scaled).astype(jnp.bfloat16)
            out[w, :, pl.ds(F + tile * TILE, TILE)] = (im * scaled).astype(jnp.bfloat16)


def spectra(begin, count, starts, raw, after, dead, cosine, sine, earlier):
    rows = raw.shape[0]
    vmem, smem = (pl.BlockSpec(memory_space=space) for space in (pltpu.VMEM, pltpu.SMEM))
    return pl.pallas_call(
        functools.partial(spectra_kernel, begin),
        in_specs=[smem] + [vmem] * 5 + [pl.BlockSpec(memory_space=pl.ANY)] * len(earlier),
        out_specs=vmem,
        scratch_shapes=[
            pltpu.VMEM((PAIRS, 2 * count * rows, SPAN), jnp.bfloat16),
            pltpu.VMEM((PAIRS, 2, 2 * count * rows, 2 * TILE), jnp.float32),
        ],
        out_shape=jax.ShapeDtypeStruct((count, rows, 2 * F), jnp.bfloat16),
        compiler_params=pltpu.CompilerParams(vmem_limit_bytes=24 << 20),
        cost_estimate=pl.CostEstimate(flops=16 * count * rows * SPAN * PAIRS * 2 * TILE, bytes_accessed=10 << 20, transcendentals=0),
        name="spectra",
    )(starts, raw, after, dead, cosine, sine, *earlier)


def correlate_kernel(final, offsets, *refs):
    blocks = refs[:4]
    table, rest = refs[4], refs[5:]
    wide, stack = rest[-2:]
    outs = rest[-4:-2] if final else rest[-3:-2]
    earlier = rest[: len(rest) - 2 - len(outs)]
    count, rows, _ = blocks[0].shape
    tiles = 2 * F // TILE
    for at, block in enumerate(blocks):
        for w in range(count):
            for tile in range(tiles):
                wide[w, tile, pl.ds(at * rows, rows), :] = block[w, :, pl.ds(tile * TILE, TILE)].astype(jnp.float32)
    group = 16

    def one_offset(o, carry):
        distance = offsets[o]
        far = distance >= 2 * rows
        mine = jnp.where(far, 0, rows)
        theirs = distance + jnp.where(far, -rows, rows)
        for part in range(rows // group):
            for tile in range(tiles // 2):
                real = jnp.zeros((group, TILE), jnp.float32)
                imag = jnp.zeros((group, TILE), jnp.float32)
                for w in range(count):
                    at = pl.multiple_of(mine + part * group, group)
                    a_re = wide[w, tile, pl.ds(at, group), :]
                    a_im = wide[w, tile + tiles // 2, pl.ds(at, group), :]
                    b_re = wide[w, tile, pl.ds(theirs + part * group, group), :]
                    b_im = wide[w, tile + tiles // 2, pl.ds(theirs + part * group, group), :]
                    real = real + a_re * b_re + a_im * b_im
                    imag = imag + a_im * b_re - a_re * b_im
                row = pl.ds(pl.multiple_of(o * rows + part * group, group), group)
                stack[row, pl.ds(tile * TILE, TILE)] = real.astype(jnp.bfloat16)
                stack[row, pl.ds(F + tile * TILE, TILE)] = imag.astype(jnp.bfloat16)
        return carry

    lax.fori_loop(0, offsets.shape[0], one_offset, 0)
    quarter = stack.shape[0] // 4
    values = []
    for part in range(4):
        row = pl.ds(part * quarter, quarter)
        value = jnp.dot(stack[row, :], table[...], preferred_element_type=jnp.float32)
        if earlier:
            value = value + earlier[0][row, :]
        if not final:
            outs[0][row, :] = value
            continue
        values.append(value * np.float32(1 / np.sqrt(4 * W_DEV * F)))
        if part % 2 == 1:
            first = lax.axis_index("tm") % 2 == 0
            row = pl.ds(part // 2 * quarter, quarter)
            outs[0][row, :] = jnp.where(first, values[-2], values[-1])
            outs[1][row, :] = jnp.where(first, values[-1], values[-2]).astype(outs[1].dtype)


def correlate(offsets, blocks, table, earlier, final):
    count, rows, _ = blocks[0].shape
    total = offsets.shape[0] * rows
    more = [] if earlier is None else [earlier]
    vmem = pl.BlockSpec(memory_space=pltpu.VMEM)
    if final:
        shapes = [jax.ShapeDtypeStruct((total // 2, LAGS), kind) for kind in (jnp.float32, jnp.bfloat16)]
    else:
        shapes = [jax.ShapeDtypeStruct((total, LAGS), jnp.float32)]
    return pl.pallas_call(
        functools.partial(correlate_kernel, final),
        in_specs=[pl.BlockSpec(memory_space=pltpu.SMEM)] + [vmem] * (5 + len(more)),
        out_specs=[vmem] * len(shapes),
        out_shape=shapes,
        scratch_shapes=[
            pltpu.VMEM((count, 2 * F // TILE, 4 * rows, TILE), jnp.float32),
            pltpu.VMEM((total, 2 * F), jnp.bfloat16),
        ],
        compiler_params=pltpu.CompilerParams(vmem_limit_bytes=24 << 20),
        cost_estimate=pl.CostEstimate(flops=2 * total * 2 * F * LAGS, bytes_accessed=8 << 20, transcendentals=0),
        name="correlate",
    )(offsets, *blocks, table, *more)


def moved(block, axis, distance):
    size = lax.axis_size(axis)
    return lax.ppermute(block, axis, [(i, i + distance) for i in range(size) if 0 <= i + distance < size])


def whole(raw, starts, dead_mask, offsets):
    rows = raw.shape[0]
    after = moved(raw[:, :HOP], "tm", -1)
    dead = dead_mask[None, :]
    cosine, sine = forward_tables()
    back = jnp.asarray(inverse_table())

    own, left, near, away = [], [], [], []
    at = 0
    for size in CHUNKS:
        own.append(spectra(at, size, starts, raw, after, dead, cosine, sine, own[-1:]))
        near.append(moved(own[-1], "chan", -1))
        left.append(moved(own[-1], "chan", 2))
        at += size
    total = None
    for c in range(len(CHUNKS)):
        away.append(moved(near[c], "chan", -1))
        blocks = [left[c], own[c], near[c], away[c]]
        total, *sent = correlate(offsets, blocks, back, total, c == len(CHUNKS) - 1)

    owners = lax.axis_size("tm")
    each = offsets.shape[0] // owners
    me = lax.axis_index("tm")
    side = me // 2
    got = lax.ppermute(sent[0], "tm", [(i, i ^ 1) for i in range(owners)])
    pair = (total + got.astype(jnp.float32)).reshape(2, each, rows, LAGS)
    sent = lax.dynamic_index_in_dim(pair, 1 - side, 0, keepdims=False).astype(jnp.bfloat16)
    kept = lax.dynamic_index_in_dim(pair, side, 0, keepdims=False)
    got = lax.ppermute(sent, "tm", [(i, i ^ 2) for i in range(owners)])
    result = kept + got.astype(jnp.float32)
    ahead = moved(result.astype(jnp.bfloat16), "chan", -2)
    mine = lax.dynamic_slice_in_dim(offsets, me * each, each)
    return jnp.where((mine >= 2 * rows)[:, None, None], ahead.astype(jnp.float32), result)


def solution(mesh):
    in_specs = (P("chan", "tm"), P("tm"), P("chan"), P())
    out_specs = P("tm", "chan", None)
    return jax.shard_map(whole, mesh=mesh, in_specs=in_specs, out_specs=out_specs, check_vma=False)
```

```python
import functools

import jax
import jax.numpy as jnp
import numpy as np
from jax import lax
from jax.experimental import pallas as pl
from jax.experimental.pallas import tpu as pltpu
from jax.sharding import PartitionSpec as P

HOP = 4096
WIN = 8192
F = 640
F0 = 16
LAGS = 256
W_DEV = 8
TILE = 128
RADIX = 8
ORDER = (1, 7, 2, 6, 3, 5, 0, 4)
SPAN = WIN // RADIX
PAIRS = RADIX // 2
PAIR = F // PAIRS
SEED = 64
CHUNKS = (4, 3, 1)


def ordered_bins():
    return np.concatenate([np.arange(F0 + branch, F0 + F, RADIX) for branch in ORDER])


def forward_tables():
    bins = ordered_bins()
    spread = np.full((PAIRS, 2 * TILE), -1)
    for pair in range(PAIRS):
        at = pair * (PAIR - TILE)
        spread[pair, at : at + PAIR] = bins[pair * PAIR : (pair + 1) * PAIR]
    spread = spread.reshape(-1)
    near = 2 * np.pi / WIN * (np.arange(SEED)[:, None] * spread[None, :] % WIN)
    far = 2 * np.pi / WIN * (SEED * np.arange(SPAN // SEED)[:, None] * spread[None, :] % WIN)
    used = spread >= 0
    c1, s1 = (jnp.asarray(part * used, jnp.float32)[None] for part in (np.cos(near), np.sin(near)))
    c2, s2 = (jnp.asarray(part, jnp.float32)[:, None] for part in (np.cos(far), np.sin(far)))
    return [part.astype(jnp.bfloat16).reshape(SPAN, -1) for part in (c1 * c2 - s1 * s2, s1 * c2 + c1 * s2)]


def inverse_table():
    bins = ordered_bins()
    lagged = np.arange(LAGS) - LAGS // 2
    angle = 2 * np.pi / WIN * (bins[:, None] * lagged[None, :] % WIN)
    return np.concatenate([np.cos(angle), -np.sin(angle)], axis=0).astype(jnp.bfloat16)


def branches(x):
    total = [x[j] + x[j + 4] for j in range(4)]
    apart = [x[j] - x[j + 4] for j in range(4)]
    even, odd = total[0] + total[2], total[1] + total[3]
    side = (apart[1] - apart[3]) * np.float32(np.sqrt(0.5))
    down = (apart[1] + apart[3]) * np.float32(np.sqrt(0.5))
    return [
        (apart[0] + side, -apart[2] - down),
        (total[0] - total[2], total[3] - total[1]),
        (apart[0] - side, apart[2] - down),
        (even + odd, even - odd),
    ]


def fold_window(start, raw, after, folded, w, count):
    rows, span = raw.shape
    last = span - WIN
    group, width = 16, 2 * TILE
    block = pl.multiple_of(start // WIN * WIN, WIN)
    inside = start % WIN
    after_block = pl.multiple_of(jnp.minimum(block + WIN, last), WIN)
    place = lax.broadcasted_iota(jnp.int32, (RADIX, SPAN), 0) * SPAN + lax.broadcasted_iota(jnp.int32, (RADIX, SPAN), 1)
    phase = (place - start) & (WIN - 1)
    hann = 0.5 - 0.5 * jnp.cos(np.float32(2 * np.pi / WIN) * phase.astype(jnp.float32))

    def fold_rows(step, carry):
        row = pl.multiple_of(step * group, group)
        for at in range(0, SPAN, width):
            lane = lax.broadcasted_iota(jnp.int32, (group, width), 1) + at
            x = []
            for j in range(RADIX):
                here = raw[pl.ds(row, group), pl.ds(block + j * SPAN + at, width)]
                later = raw[pl.ds(row, group), pl.ds(after_block + j * SPAN + at, width)]
                if after is not None and j * SPAN < HOP:
                    later = jnp.where(block == last, after[pl.ds(row, group), pl.ds(j * SPAN + at, width)], later)
                picked = jnp.where(lane >= inside - j * SPAN, here.astype(jnp.float32), later.astype(jnp.float32))
                picked = picked * hann[j : j + 1, at : at + width]
                x.append(picked.astype(jnp.bfloat16).astype(jnp.float32))
            for pair, values in enumerate(branches(x)):
                for part, value in enumerate(values):
                    to = pl.multiple_of((part * count + w) * rows + row, group)
                    folded[pair, pl.ds(to, group), pl.ds(at, width)] = value.astype(jnp.bfloat16)
        return carry

    lax.fori_loop(0, rows // group, fold_rows, 0)


def fold_kernel(starts, raw, _, folded):
    last = raw.shape[1] - WIN
    count = folded.shape[1] // (2 * raw.shape[0])

    def one_window(w, carry):
        @pl.when(starts[w] <= last)
        def _():
            fold_window(starts[w], raw, None, folded, w, count)

        return carry

    lax.fori_loop(0, count, one_window, 0)


def fold(count, starts, raw, table):
    smem, vmem = (pl.BlockSpec(memory_space=space) for space in (pltpu.SMEM, pltpu.VMEM))
    rows = raw.shape[0]
    return pl.pallas_call(
        fold_kernel,
        in_specs=[smem, vmem, pl.BlockSpec(memory_space=pl.ANY)],
        out_specs=vmem,
        out_shape=jax.ShapeDtypeStruct((PAIRS, 2 * count * rows, SPAN), jnp.bfloat16),
        compiler_params=pltpu.CompilerParams(vmem_limit_bytes=24 << 20),
        cost_estimate=pl.CostEstimate(flops=24 * count * rows * WIN, bytes_accessed=10 << 20, transcendentals=0),
        name="fold",
    )(starts, raw, table)


def spectra_kernel(begin, ready, starts, raw, after, dead, cosine, sine, *refs):
    out, folded, product = refs[-3:]
    rows, span = raw.shape
    count = out.shape[0]
    width = 2 * TILE

    def one_window(w, carry):
        start = starts[begin + w]
        if ready:

            @pl.when(start > span - WIN)
            def _():
                fold_window(start, raw, after, folded, w, count)

        else:
            fold_window(start, raw, after, folded, w, count)
        return carry

    lax.fori_loop(0, count, one_window, 0)
    for pair in range(PAIRS):
        columns = slice(pair * width, (pair + 1) * width)
        product[pair, 0] = jnp.dot(folded[pair], cosine[:, columns], preferred_element_type=jnp.float32)
        product[pair, 1] = jnp.dot(folded[pair], sine[:, columns], preferred_element_type=jnp.float32)

    square = lax.broadcasted_iota(jnp.int32, (rows, rows), 0) == lax.broadcasted_iota(jnp.int32, (rows, rows), 1)
    live = jnp.sum(jnp.where(square, dead[...].astype(jnp.float32), 0.0), axis=1, keepdims=True)
    lane = lax.broadcasted_iota(jnp.int32, (1, width), 1)
    for w in range(count):
        first, second = pl.ds(w * rows, rows), pl.ds((count + w) * rows, rows)
        reals, imags = [], []
        for pair in range(PAIRS):
            leading = lane < pair * (PAIR - TILE) + PAIR // 2
            c_first, c_second = product[pair, 0, first, :], product[pair, 0, second, :]
            s_first, s_second = product[pair, 1, first, :], product[pair, 1, second, :]
            if pair < PAIRS - 1:
                reals.append(c_first + jnp.where(leading, s_second, -s_second))
                imags.append(jnp.where(leading, c_second, -c_second) - s_first)
            else:
                reals.append(jnp.where(leading, c_first, c_second))
                imags.append(-jnp.where(leading, s_first, s_second))
        tiles = [[], []]
        for into, parts in zip(tiles, (reals, imags)):
            into.append(parts[0][:, :TILE])
            for pair in range(1, PAIRS):
                into.append(parts[pair - 1][:, TILE:] + parts[pair][:, :TILE])
            into.append(parts[-1][:, TILE:])
        sizes = [jnp.sqrt(re * re + im * im) for re, im in zip(*tiles)]
        level = jnp.sum(sum(sizes[1:], sizes[0]), axis=-1, keepdims=True) * np.float32(1 / F)
        for tile, (re, im, amplitude) in enumerate(zip(*tiles, sizes)):
            scaled = live / (amplitude + 0.1 * level + 1e-06)
            out[w, :, pl.ds(tile * TILE, TILE)] = (re * scaled).astype(jnp.bfloat16)
            out[w, :, pl.ds(F + tile * TILE, TILE)] = (im * scaled).astype(jnp.bfloat16)


def spectra(begin, count, starts, raw, after, dead, cosine, sine, earlier, ready=None):
    rows = raw.shape[0]
    vmem, smem = (pl.BlockSpec(memory_space=space) for space in (pltpu.VMEM, pltpu.SMEM))
    operands = [starts, raw, after, dead, cosine, sine, *earlier]
    in_specs = [smem] + [vmem] * 5 + [pl.BlockSpec(memory_space=pl.ANY)] * len(earlier)
    shapes = [jax.ShapeDtypeStruct((count, rows, 2 * F), jnp.bfloat16)]
    parts = (PAIRS, 2 * count * rows, SPAN)
    scratch = [pltpu.VMEM((PAIRS, 2, 2 * count * rows, 2 * TILE), jnp.float32)]
    aliases = {}
    if ready is None:
        scratch.insert(0, pltpu.VMEM(parts, jnp.bfloat16))
    else:
        aliases[len(operands)] = 1
        operands.append(ready)
        in_specs.append(vmem)
        shapes.append(jax.ShapeDtypeStruct(parts, jnp.bfloat16))
    return pl.pallas_call(
        functools.partial(spectra_kernel, begin, ready is not None),
        in_specs=in_specs,
        out_specs=[vmem] * len(shapes),
        scratch_shapes=scratch,
        out_shape=shapes,
        input_output_aliases=aliases,
        compiler_params=pltpu.CompilerParams(vmem_limit_bytes=24 << 20),
        cost_estimate=pl.CostEstimate(flops=16 * count * rows * SPAN * PAIRS * 2 * TILE, bytes_accessed=10 << 20, transcendentals=0),
        name="spectra",
    )(*operands)[0]


def correlate_kernel(final, offsets, *refs):
    blocks = refs[:4]
    table, rest = refs[4], refs[5:]
    wide, stack = rest[-2:]
    outs = rest[-4:-2] if final else rest[-3:-2]
    earlier = rest[: len(rest) - 2 - len(outs)]
    count, rows, _ = blocks[0].shape
    tiles = 2 * F // TILE
    for at, block in enumerate(blocks):
        for w in range(count):
            for tile in range(tiles):
                wide[w, tile, pl.ds(at * rows, rows), :] = block[w, :, pl.ds(tile * TILE, TILE)].astype(jnp.float32)
    group = 16

    def one_offset(o, carry):
        distance = offsets[o]
        far = distance >= 2 * rows
        mine = jnp.where(far, 0, rows)
        theirs = distance + jnp.where(far, -rows, rows)
        for part in range(rows // group):
            for tile in range(tiles // 2):
                real = jnp.zeros((group, TILE), jnp.float32)
                imag = jnp.zeros((group, TILE), jnp.float32)
                for w in range(count):
                    at = pl.multiple_of(mine + part * group, group)
                    a_re = wide[w, tile, pl.ds(at, group), :]
                    a_im = wide[w, tile + tiles // 2, pl.ds(at, group), :]
                    b_re = wide[w, tile, pl.ds(theirs + part * group, group), :]
                    b_im = wide[w, tile + tiles // 2, pl.ds(theirs + part * group, group), :]
                    real = real + a_re * b_re + a_im * b_im
                    imag = imag + a_im * b_re - a_re * b_im
                row = pl.ds(pl.multiple_of(o * rows + part * group, group), group)
                stack[row, pl.ds(tile * TILE, TILE)] = real.astype(jnp.bfloat16)
                stack[row, pl.ds(F + tile * TILE, TILE)] = imag.astype(jnp.bfloat16)
        return carry

    lax.fori_loop(0, offsets.shape[0], one_offset, 0)
    quarter = stack.shape[0] // 4
    values = []
    for part in range(4):
        row = pl.ds(part * quarter, quarter)
        value = jnp.dot(stack[row, :], table[...], preferred_element_type=jnp.float32)
        if earlier:
            value = value + earlier[0][row, :]
        if not final:
            outs[0][row, :] = value
            continue
        values.append(value * np.float32(1 / np.sqrt(4 * W_DEV * F)))
        if part % 2 == 1:
            first = lax.axis_index("tm") % 2 == 0
            row = pl.ds(part // 2 * quarter, quarter)
            outs[0][row, :] = jnp.where(first, values[-2], values[-1])
            outs[1][row, :] = jnp.where(first, values[-1], values[-2]).astype(outs[1].dtype)


def correlate(offsets, blocks, table, earlier, final):
    count, rows, _ = blocks[0].shape
    total = offsets.shape[0] * rows
    more = [] if earlier is None else [earlier]
    vmem = pl.BlockSpec(memory_space=pltpu.VMEM)
    if final:
        shapes = [jax.ShapeDtypeStruct((total // 2, LAGS), kind) for kind in (jnp.float32, jnp.bfloat16)]
    else:
        shapes = [jax.ShapeDtypeStruct((total, LAGS), jnp.float32)]
    return pl.pallas_call(
        functools.partial(correlate_kernel, final),
        in_specs=[pl.BlockSpec(memory_space=pltpu.SMEM)] + [vmem] * (5 + len(more)),
        out_specs=[vmem] * len(shapes),
        out_shape=shapes,
        scratch_shapes=[
            pltpu.VMEM((count, 2 * F // TILE, 4 * rows, TILE), jnp.float32),
            pltpu.VMEM((total, 2 * F), jnp.bfloat16),
        ],
        compiler_params=pltpu.CompilerParams(vmem_limit_bytes=24 << 20),
        cost_estimate=pl.CostEstimate(flops=2 * total * 2 * F * LAGS, bytes_accessed=8 << 20, transcendentals=0),
        name="correlate",
    )(offsets, *blocks, table, *more)


def moved(block, axis, distance):
    size = lax.axis_size(axis)
    return lax.ppermute(block, axis, [(i, i + distance) for i in range(size) if 0 <= i + distance < size])


def whole(raw, starts, dead_mask, offsets):
    rows = raw.shape[0]
    after = moved(raw[:, :HOP], "tm", -1)
    dead = dead_mask[None, :]
    cosine, sine = forward_tables()
    ready = fold(CHUNKS[0], starts, raw, cosine)
    back = jnp.asarray(inverse_table())

    own, left, near, away = [], [], [], []
    at = 0
    for size in CHUNKS:
        own.append(spectra(at, size, starts, raw, after, dead, cosine, sine, own[-1:], None if own else ready))
        near.append(moved(own[-1], "chan", -1))
        left.append(moved(own[-1], "chan", 2))
        at += size
    total = None
    for c in range(len(CHUNKS)):
        away.append(moved(near[c], "chan", -1))
        blocks = [left[c], own[c], near[c], away[c]]
        total, *sent = correlate(offsets, blocks, back, total, c == len(CHUNKS) - 1)

    owners = lax.axis_size("tm")
    each = offsets.shape[0] // owners
    me = lax.axis_index("tm")
    side = me // 2
    got = lax.ppermute(sent[0], "tm", [(i, i ^ 1) for i in range(owners)])
    pair = (total + got.astype(jnp.float32)).reshape(2, each, rows, LAGS)
    sent = lax.dynamic_index_in_dim(pair, 1 - side, 0, keepdims=False).astype(jnp.bfloat16)
    kept = lax.dynamic_index_in_dim(pair, side, 0, keepdims=False)
    got = lax.ppermute(sent, "tm", [(i, i ^ 2) for i in range(owners)])
    result = kept + got.astype(jnp.float32)
    ahead = moved(result.astype(jnp.bfloat16), "chan", -2)
    mine = lax.dynamic_slice_in_dim(offsets, me * each, each)
    return jnp.where((mine >= 2 * rows)[:, None, None], ahead.astype(jnp.float32), result)


def solution(mesh):
    in_specs = (P("chan", "tm"), P("tm"), P("chan"), P())
    out_specs = P("tm", "chan", None)
    return jax.shard_map(whole, mesh=mesh, in_specs=in_specs, out_specs=out_specs, check_vma=False)
```
